512 devices in a mesh: aux: 16 (over z_lo, y), row: 32 (over x, z_hi, core).
Axes of the slice: x: 4, y: 4, z: 16 (z_hi: 4, z_lo: 4; z = z_hi * 4 + z_lo), core: 2. Of those that a mesh axis runs over, the one named last changes fastest.
Arguments:
- coeff: bfloat16 [800, 4096], P(None, 'row'), may hold values from -0.109375 to 0.109375
- band: bfloat16 [32, 384, 4096], P('aux', None, 'row'), may hold values from -6 to 6
- pairs: int32 [32, 32], replicated, may hold values from 0 to 1, as said below
Outputs:
- exchange_k: float32 [4096, 4096], P('row', 'aux')
The draws below stay inside these ranges and needn't reach their ends.
Inputs may be any that keep to these rules, and one draw needn't show every extreme that they name: pairs is symmetric, holds only 0 and 1, and its diagonal is 1; how many blocks a row keeps differs from row to row.
All inputs are finite; a program needn't handle non-finite values.
Results may differ from the reference program's by a relative error of at most 0.0012.
Values may be sent and summed in bfloat16 or wider, within the bound.
No kernel may reach another device: no remote copies, remote signals or barrier semaphores. Data moves between devices by JAX's collectives and lax.ppermute only.
A program may use at most 64 MiB of HBM per device.

```python
import jax
import jax.numpy as jnp
from jax import lax

BLK = 128
NOCC = 800
NBLK = 32
NBF = 4096
NAUX = 32


def draw_pairs(key, part):
    key_density, key_ticket = jax.random.split(jax.random.fold_in(key, 7))
    density = jax.random.randint(key_density, (NBLK,), 5, 50)
    ticket = jax.random.randint(key_ticket, (NBLK, NBLK), 0, 100)
    chosen = ticket < density[:, None] + density[None, :]
    positions = jnp.arange(NBLK)
    strict = positions[None, :] > positions[:, None]
    one_side = jnp.where(strict & chosen, 1, 0).astype(jnp.int32)
    return (one_side + one_side.T + jnp.eye(NBLK, dtype=jnp.int32)).astype(jnp.int32)


def shard_levels(key, shape, cuts, least, top_value):
    gain = 1.0
    for position, blocks in cuts:
        heights = jax.random.uniform(jax.random.fold_in(jax.random.fold_in(key, 6), position), (blocks,), jnp.float32, least / len(cuts), top_value / len(cuts))
        gain = gain * jnp.repeat(jnp.exp(heights), shape[position] // blocks).reshape((-1,) + (1,) * (len(shape) - 1 - position))
    return gain


def normal_values(rng, shape, spread, most, cuts=(), kind=jnp.bfloat16):
    level = shard_levels(rng, shape, cuts, -0.22, 0.18) if cuts else 1.0
    result = jax.random.normal(rng, shape, jnp.float32) * spread * level
    return jnp.minimum(jnp.maximum(result, -most), most).astype(kind)


def setup_inputs(seed: int = 0) -> dict:
    keys = jax.random.split(jax.random.key(seed), 4)
    coeff = normal_values(keys[0], (NOCC, NBF), (3 * BLK * 8) ** -0.5, 0.109375, ((1, 32),))
    band = normal_values(keys[1], (NAUX, 3 * BLK, NBF), 1.0, 6.0, ((0, 16), (2, 32)))
    pairs = draw_pairs(jax.random.fold_in(keys[3], 71), 0)
    return dict(coeff=coeff, band=band, pairs=pairs)


def reference(coeff, band, pairs):
    padded = jnp.pad(coeff.astype(jnp.float32), ((0, 0), (BLK, BLK)))
    factors = []
    for block_index in range(NBLK):
        window = padded[:, block_index * BLK:(block_index + 3) * BLK]
        slab_part = band[:, :, block_index * BLK:(block_index + 1) * BLK].astype(jnp.float32)
        product = jnp.einsum("ij,qjm->qim", window, slab_part, precision=lax.Precision.HIGHEST)
        factors.append(product.astype(jnp.bfloat16))
    half_factor = jnp.concatenate(factors, axis=2).reshape(-1, NBF).astype(jnp.float32)
    complete = lax.dot_general(half_factor, half_factor, (((0,), (0,)), ((), ())), precision=lax.Precision.HIGHEST, preferred_element_type=jnp.float32)
    screen = jnp.repeat(jnp.repeat(pairs, BLK, axis=0), BLK, axis=1).astype(jnp.float32)
    return complete * screen
```

```python
import math

import jax
import jax.numpy as jnp
from jax import lax
from jax.experimental import pallas as pl
from jax.experimental.pallas import tpu as pltpu
from jax.sharding import Mesh
from jax.sharding import PartitionSpec as P


AUX = ("zl", "y")
ROW = ("x", "zh", "c")
ALONG_Z = [(4 * zl + zh, 4 * zl + (zh + (1, 3)[zl % 2]) % 4) for zl in range(4) for zh in range(4)]


def shifted(value, axis, step):
    count = lax.axis_size(axis)
    return lax.ppermute(value, axis, [(i, (i + step) % count) for i in range(count)])


def is_even():
    return lax.rem(lax.axis_index("zl"), 2) == 0


def own_part(coeff, band, sides, made):
    block = coeff.shape[1]
    start = 2 * block * lax.axis_index("c")
    for row, side in enumerate((start, 2 * block - start)):
        for q in range(2):
            sides[row * block : (row + 1) * block, q * block : (q + 1) * block] = band[
                q, pl.ds(side, block)
            ]
    middle = jnp.concatenate([band[q, block : 2 * block] for q in range(2)], axis=1)
    made[...] = jnp.dot(coeff[...], middle, preferred_element_type=jnp.float32)


def half_block(outer, partner, sides, made, half, copies, sems):
    nocc, block = outer.shape
    window = jnp.concatenate([outer[...], partner[...]], axis=1)
    whole = made[...] + jnp.dot(window, sides[...], preferred_element_type=jnp.float32)
    for q in range(2):
        half[q * nocc : (q + 1) * nocc] = whole[:, q * block : (q + 1) * block].astype(half.dtype)
    sent = [pltpu.make_async_copy(half, copies.at[k], sems.at[k]) for k in range(4)]
    for copy in sent:
        copy.start()
    for copy in sent:
        copy.wait()


def kept_out(kernel):
    def run(*refs):
        *inputs, out, made, sem = refs
        kernel(*inputs, made)
        copy = pltpu.make_async_copy(made, out, sem)
        copy.start()
        copy.wait()

    return run


def tiles_of(columns, mine):
    block = mine.shape[2]
    made = lax.dot_general(
        jnp.concatenate([column[...] for column in columns], axis=1),
        jnp.concatenate([mine[k] for k in range(4)], axis=1),
        (((0,), (0,)), ((), ())),
        preferred_element_type=jnp.float32,
    )
    for k in range(4):
        yield (
            k,
            [
                made[j * block : (j + 1) * block, k * block : (k + 1) * block]
                for j in range(len(columns))
            ],
        )


def by_parity(store, tile):
    even = is_even()
    pl.when(even)(lambda: store(tile))
    pl.when(jnp.logical_not(even))(lambda: store(tile.T))


def first_tiles(own_other, near, near_other, mine, slices):
    cut = slices.shape[4]
    core = lax.axis_index("c")
    own = mine.at[lax.axis_index("x")]
    for k, made in tiles_of((own, own_other, near, near_other), mine):
        for side in range(2):

            def put(kind, tile, to=(core + side) % 2, k=k):
                for s in range(4):
                    slices[s, to, kind, k] = tile[s * cut : (s + 1) * cut]

            put(0, made[side])
            by_parity(lambda tile, put=put: put(1, tile), made[2 + side])


def patch_tiles(near, near_other, far, far_other, mine, patch):
    cut = patch.shape[4]
    core = lax.axis_index("c")
    for k, made in tiles_of((near, near_other, far, far_other), mine):
        for side in range(2):

            def put(kind, tile, of=(core + side) % 2, k=k):
                for s in range(4):
                    patch[s, k, kind, of] = tile[s * cut : (s + 1) * cut]

            put(1, made[2 + side])
            by_parity(lambda tile, put=put: put(0, tile), made[side])


def near_summed(early, out):
    for c in range(2):
        for k in range(4):
            out[c, k] = early[0, c, 1, k] + early[1, c, 1, k] + early[2, c, 1, k] + early[3, c, 1, k]


def placed(early, mirrored, arrived, parts):
    zh = lax.axis_index("zh")
    toward = jnp.where(is_even(), 3, 1)
    homes = (lax.rem(zh + toward, 4), lax.rem(zh + 2, 4))
    for j in range(4):
        for c in range(2):
            parts[j, zh, c] = early[0, c, 0, j] + early[1, c, 0, j] + early[2, c, 0, j] + early[3, c, 0, j]
            parts[j, lax.rem(zh + 4 - toward, 4), c] = mirrored[c, j]
            for kind in range(2):
                parts[j, homes[kind], c] = (
                    arrived[0, j, kind, c]
                    + arrived[1, j, kind, c]
                    + arrived[2, j, kind, c]
                    + arrived[3, j, kind, c]
                )


def finished(pairs, total, out):
    block = out.shape[0]
    row = 8 * lax.axis_index("x") + 2 * lax.axis_index("zh") + lax.axis_index("c")
    first = 8 * lax.axis_index("zl") + 2 * lax.axis_index("y")
    straight = lax.rem(lax.axis_index("y") + 4 - lax.axis_index("zh"), 4) < 2
    for c in range(2):
        keep = pairs[row, first + c].astype(jnp.float32)
        tile = (total[0, :, c] + total[1, :, c] + total[2, :, c] + total[3, :, c]) * keep
        tile = tile.reshape(block, block)

        @pl.when(straight)
        def _(tile=tile, c=c):
            out[:, c * block : (c + 1) * block] = tile

        @pl.when(jnp.logical_not(straight))
        def _(tile=tile, c=c):
            out[:, c * block : (c + 1) * block] = tile.T


def local(kernel, results, flops, *arrays, scalars=0, out=False):
    whole = pl.BlockSpec(memory_space=pltpu.VMEM)
    table = pl.BlockSpec(memory_space=pltpu.SMEM)
    shapes = [
        pltpu.HBM(shape, kind) if space == pltpu.HBM else jax.ShapeDtypeStruct(shape, kind)
        for shape, kind, space in results
    ]
    scratch = []
    if out:
        kernel = kept_out(kernel)
        scratch = [pltpu.VMEM(*results[0][:2]), pltpu.SemaphoreType.DMA(())]
    elif any(space == pltpu.HBM for *_, space in results):
        scratch = [pltpu.SemaphoreType.DMA((4,))]
    moved = sum(a.size * a.dtype.itemsize for a in arrays)
    moved += sum(math.prod(shape) * jnp.dtype(kind).itemsize for shape, kind, _ in results)
    return pl.pallas_call(
        kernel,
        out_shape=shapes,
        in_specs=[table] * scalars + [whole] * (len(arrays) - scalars),
        out_specs=[pl.BlockSpec(memory_space=space) for *_, space in results],
        scratch_shapes=scratch,
        cost_estimate=pl.CostEstimate(flops=flops, bytes_accessed=moved, transcendentals=0),
        compiler_params=pltpu.CompilerParams(vmem_limit_bytes=2 * moved + (8 << 20)),
    )(*arrays)


def patch_sums(coeff, band, pairs):
    nocc, block = coeff.shape
    cut = block // 4

    count = lax.axis_size(ROW)
    partner = shifted(coeff, "c", 1)
    outward = [(r, r + 1) for r in range(1, count - 1, 2)]
    outer = lax.ppermute(coeff, ROW, outward + [(b, a) for a, b in outward])
    depth = band.shape[0] * nocc
    wide = band.shape[0] * block
    vmem, hbm = pltpu.VMEM, pltpu.HBM
    sides, made = local(
        own_part,
        [((2 * block, wide), jnp.bfloat16, vmem), ((nocc, wide), jnp.float32, vmem)],
        2 * nocc * block * wide,
        coeff,
        band,
    )
    half, copies = local(
        half_block,
        [((depth, block), jnp.bfloat16, vmem), ((4, depth, block), jnp.bfloat16, hbm)],
        4 * nocc * block * wide,
        outer,
        partner,
        sides,
        made,
    )

    near = lax.ppermute(half, ("zl", "zh"), ALONG_Z)
    mine = lax.all_to_all(copies, "x", split_axis=0, concat_axis=0, tiled=True)
    own_other = shifted(half, "c", 1)
    far = lax.ppermute(near, ("zl", "zh"), ALONG_Z)
    near_other = shifted(near, "c", 1)
    far_other = shifted(far, "c", 1)

    def summed(tiles, axes):
        return lax.all_to_all(tiles, axes, split_axis=0, concat_axis=0, tiled=True)

    work = 2 * half.shape[0] * block * 16 * block
    (slices,) = local(
        first_tiles,
        [((4, 2, 2, 4, cut, block), jnp.float32, hbm)],
        work,
        own_other,
        near,
        near_other,
        mine,
        out=True,
    )
    early = summed(slices.reshape(8, 8 * cut, block), ("y", "c"))
    early = early.reshape(4, 2, 2, 4, cut, block)
    (mirrored,) = local(near_summed, [((2, 4, cut, block), jnp.float32, vmem)], 0, early)
    mirrored = lax.ppermute(mirrored, ("zl", "zh"), [(b, a) for a, b in ALONG_Z])
    (patch,) = local(
        patch_tiles,
        [((4, 4, 2, 2, cut, block), jnp.float32, hbm)],
        work,
        near,
        near_other,
        far,
        far_other,
        mine,
        out=True,
    )
    arrived = summed(patch.reshape(16, 4 * cut, block), ("y", "x"))
    arrived = arrived.reshape(4, 4, 2, 2, cut, block)
    (parts,) = local(
        placed, [((4, 4, 2, cut, block), jnp.float32, vmem)], 0, early, mirrored, arrived
    )
    total = lax.all_to_all(
        parts.reshape(16, 2 * cut, block), AUX, split_axis=0, concat_axis=0, tiled=True
    )
    total = total.reshape(4, 4, 2, cut, block)
    (out,) = local(
        finished, [((block, 2 * block), jnp.float32, vmem)], 0, pairs, total, scalars=1
    )
    return out


def solution(mesh):
    torus = Mesh(mesh.devices.reshape(4, 4, 4, 4, 2), ("zl", "y", "x", "zh", "c"))
    in_specs = (P(None, ROW), P(AUX, None, ROW), P())
    return jax.shard_map(
        patch_sums, mesh=torus, in_specs=in_specs, out_specs=P(ROW, AUX), check_vma=False
    )
```

```python
import math

import jax
import jax.numpy as jnp
from jax import lax
from jax.experimental import pallas as pl
from jax.experimental.pallas import tpu as pltpu
from jax.sharding import Mesh
from jax.sharding import PartitionSpec as P


AUX = ("zl", "y")
ROW = ("x", "zh", "c")
ALONG_Z = [(4 * zl + zh, 4 * zl + (zh + (1, 3)[zl % 2]) % 4) for zl in range(4) for zh in range(4)]


def shifted(value, axis, step):
    count = lax.axis_size(axis)
    return lax.ppermute(value, axis, [(i, (i + step) % count) for i in range(count)])


def is_even():
    return lax.rem(lax.axis_index("zl"), 2) == 0


def own_part(coeff, band, sides, made):
    block = coeff.shape[1]
    start = 2 * block * lax.axis_index("c")
    for row, side in enumerate((start, 2 * block - start)):
        for q in range(2):
            sides[row * block : (row + 1) * block, q * block : (q + 1) * block] = band[
                q, pl.ds(side, block)
            ]
    middle = jnp.concatenate([band[q, block : 2 * block] for q in range(2)], axis=1)
    made[...] = jnp.dot(coeff[...], middle, preferred_element_type=jnp.float32)


def half_block(outer, partner, sides, made, half, copies, sems):
    nocc, block = outer.shape
    window = jnp.concatenate([outer[...], partner[...]], axis=1)
    whole = made[...] + jnp.dot(window, sides[...], preferred_element_type=jnp.float32)
    for q in range(2):
        half[q * nocc : (q + 1) * nocc] = whole[:, q * block : (q + 1) * block].astype(half.dtype)
    carried(*((half, copies.at[k], sems.at[k]) for k in range(4)))


def carried(*moves):
    copies = [pltpu.make_async_copy(*move) for move in moves]
    for copy in copies:
        copy.start()
    for copy in copies:
        copy.wait()


def tiles_of(columns, mine):
    block = mine.shape[2]
    made = lax.dot_general(
        jnp.concatenate([column[...] for column in columns], axis=1),
        jnp.concatenate([mine[k] for k in range(4)], axis=1),
        (((0,), (0,)), ((), ())),
        preferred_element_type=jnp.float32,
    )
    for k in range(4):
        yield (
            k,
            [
                made[j * block : (j + 1) * block, k * block : (k + 1) * block]
                for j in range(len(columns))
            ],
        )


def by_parity(store, tile):
    even = is_even()
    pl.when(even)(lambda: store(tile))
    pl.when(jnp.logical_not(even))(lambda: store(tile.T))


def first_tiles(own_other, near, near_other, mine, slices, patch, made, near_made, sems):
    cut = made.shape[4]
    core = lax.axis_index("c")
    own = mine.at[lax.axis_index("x")]
    for k, tiles in tiles_of((own, own_other, near, near_other), mine):
        for side in range(2):
            at = (core + side) % 2

            def put(tile, at=at, k=k):
                for s in range(4):
                    made[s, at, 1, k] = tile[s * cut : (s + 1) * cut]
                    near_made[s, k, at] = tile[s * cut : (s + 1) * cut]

            for s in range(4):
                made[s, at, 0, k] = tiles[side][s * cut : (s + 1) * cut]
            by_parity(put, tiles[2 + side])
    carried((made, slices, sems.at[0]), (near_made, patch.at[:, :, 0], sems.at[1]))


def far_tiles(far, far_other, mine, patch, whole, made, sems):
    cut = made.shape[3]
    core = lax.axis_index("c")
    for k, tiles in tiles_of((far, far_other), mine):
        for side in range(2):
            for s in range(4):
                made[s, k, (core + side) % 2] = tiles[side][s * cut : (s + 1) * cut]
    carried((made, whole.at[:, :, 1], sems.at[0]))


def near_summed(early, out):
    for c in range(2):
        for k in range(4):
            out[c, k] = early[0, c, 1, k] + early[1, c, 1, k] + early[2, c, 1, k] + early[3, c, 1, k]


def placed(early, mirrored, arrived, parts):
    zh = lax.axis_index("zh")
    toward = jnp.where(is_even(), 3, 1)
    homes = (lax.rem(zh + toward, 4), lax.rem(zh + 2, 4))
    for j in range(4):
        for c in range(2):
            parts[j, zh, c] = early[0, c, 0, j] + early[1, c, 0, j] + early[2, c, 0, j] + early[3, c, 0, j]
            parts[j, lax.rem(zh + 4 - toward, 4), c] = mirrored[c, j]
            for kind in range(2):
                parts[j, homes[kind], c] = (
                    arrived[0, j, kind, c]
                    + arrived[1, j, kind, c]
                    + arrived[2, j, kind, c]
                    + arrived[3, j, kind, c]
                )


def finished(pairs, total, out):
    block = out.shape[0]
    row = 8 * lax.axis_index("x") + 2 * lax.axis_index("zh") + lax.axis_index("c")
    first = 8 * lax.axis_index("zl") + 2 * lax.axis_index("y")
    straight = lax.rem(lax.axis_index("y") + 4 - lax.axis_index("zh"), 4) < 2
    kept = pairs[pl.ds(row, 1), :].astype(jnp.float32)
    places = lax.broadcasted_iota(jnp.int32, kept.shape, 1)
    for c in range(2):
        keep = jnp.sum(jnp.where(places == first + c, kept, 0.0), axis=1, keepdims=True)
        tile = total[0, :, c] + total[1, :, c] + total[2, :, c] + total[3, :, c]
        tile = tile.reshape(block, block) * keep

        @pl.when(straight)
        def _(tile=tile, c=c):
            out[:, c * block : (c + 1) * block] = tile

        @pl.when(jnp.logical_not(straight))
        def _(tile=tile, c=c):
            out[:, c * block : (c + 1) * block] = tile.T


def local(kernel, results, flops, *arrays, scratch=(), filled=False):
    specs = [pl.BlockSpec(memory_space=pltpu.VMEM)] * len(arrays)
    if filled:
        specs[-1] = pl.BlockSpec(memory_space=pltpu.HBM)
    shapes = [
        pltpu.HBM(shape, kind) if space == pltpu.HBM else jax.ShapeDtypeStruct(shape, kind)
        for shape, kind, space in results
    ]
    buffers = [pltpu.VMEM(shape, jnp.float32) for shape in scratch]
    if any(space == pltpu.HBM for *_, space in results):
        buffers.append(pltpu.SemaphoreType.DMA((4,)))
    moved = sum(a.size * a.dtype.itemsize for a in arrays)
    moved += sum(math.prod(shape) * jnp.dtype(kind).itemsize for shape, kind, _ in results)
    return pl.pallas_call(
        kernel,
        out_shape=shapes,
        in_specs=specs,
        out_specs=[pl.BlockSpec(memory_space=space) for *_, space in results],
        scratch_shapes=buffers,
        input_output_aliases={len(arrays) - 1: 0} if filled else {},
        cost_estimate=pl.CostEstimate(flops=flops, bytes_accessed=moved, transcendentals=0),
        compiler_params=pltpu.CompilerParams(vmem_limit_bytes=2 * moved + (8 << 20)),
    )(*arrays)


def patch_sums(coeff, band, pairs):
    nocc, block = coeff.shape
    cut = block // 4

    count = lax.axis_size(ROW)
    partner = shifted(coeff, "c", 1)
    outward = [(r, r + 1) for r in range(1, count - 1, 2)]
    outer = lax.ppermute(coeff, ROW, outward + [(b, a) for a, b in outward])
    depth = band.shape[0] * nocc
    wide = band.shape[0] * block
    vmem, hbm = pltpu.VMEM, pltpu.HBM
    sides, made = local(
        own_part,
        [((2 * block, wide), jnp.bfloat16, vmem), ((nocc, wide), jnp.float32, vmem)],
        2 * nocc * block * wide,
        coeff,
        band,
    )
    half, copies = local(
        half_block,
        [((depth, block), jnp.bfloat16, vmem), ((4, depth, block), jnp.bfloat16, hbm)],
        4 * nocc * block * wide,
        outer,
        partner,
        sides,
        made,
    )

    near = lax.ppermute(half, ("zl", "zh"), ALONG_Z)
    mine = lax.all_to_all(copies, "x", split_axis=0, concat_axis=0, tiled=True)
    own_other = shifted(half, "c", 1)
    far = lax.ppermute(near, ("zl", "zh"), ALONG_Z)
    near_other = shifted(near, "c", 1)
    far_other = shifted(far, "c", 1)

    def summed(tiles, axes):
        return lax.all_to_all(tiles, axes, split_axis=0, concat_axis=0, tiled=True)

    work = 2 * depth * block * 8 * block
    patch_shape = (4, 4, 2, 2, cut, block)
    slices, patch = local(
        first_tiles,
        [((4, 2, 2, 4, cut, block), jnp.float32, hbm), (patch_shape, jnp.float32, hbm)],
        2 * work,
        own_other,
        near,
        near_other,
        mine,
        scratch=[(4, 2, 2, 4, cut, block), (4, 4, 2, cut, block)],
    )
    early = summed(slices.reshape(8, 8 * cut, block), ("y", "c"))
    early = early.reshape(4, 2, 2, 4, cut, block)
    (mirrored,) = local(near_summed, [((2, 4, cut, block), jnp.float32, vmem)], 0, early)
    mirrored = lax.ppermute(mirrored, ("zl", "zh"), [(b, a) for a, b in ALONG_Z])
    (patch,) = local(
        far_tiles,
        [(patch_shape, jnp.float32, hbm)],
        work,
        far,
        far_other,
        mine,
        patch,
        scratch=[(4, 4, 2, cut, block)],
        filled=True,
    )
    arrived = summed(patch.reshape(16, 4 * cut, block), ("y", "x"))
    arrived = arrived.reshape(4, 4, 2, 2, cut, block)
    (parts,) = local(
        placed, [((4, 4, 2, cut, block), jnp.float32, vmem)], 0, early, mirrored, arrived
    )
    total = lax.all_to_all(
        parts.reshape(16, 2 * cut, block), AUX, split_axis=0, concat_axis=0, tiled=True
    )
    total = total.reshape(4, 4, 2, cut, block)
    (out,) = local(
        finished, [((block, 2 * block), jnp.float32, vmem)], 0, pairs, total
    )
    return out


def solution(mesh):
    torus = Mesh(mesh.devices.reshape(4, 4, 4, 4, 2), ("zl", "y", "x", "zh", "c"))
    in_specs = (P(None, ROW), P(AUX, None, ROW), P())
    return jax.shard_map(
        patch_sums, mesh=torus, in_specs=in_specs, out_specs=P(ROW, AUX), check_vma=False
    )
```

```python
import math

import jax
import jax.numpy as jnp
from jax import lax
from jax.experimental import pallas as pl
from jax.experimental.pallas import tpu as pltpu
from jax.sharding import Mesh
from jax.sharding import PartitionSpec as P


AUX = ("zl", "y")
ROW = ("x", "zh", "c")
ALONG_Z = [(4 * zl + zh, 4 * zl + (zh + (1, 3)[zl % 2]) % 4) for zl in range(4) for zh in range(4)]


def shifted(value, axis, step):
    count = lax.axis_size(axis)
    return lax.ppermute(value, axis, [(i, (i + step) % count) for i in range(count)])


def is_even():
    return lax.rem(lax.axis_index("zl"), 2) == 0


def own_part(coeff, band, sides, made):
    block = coeff.shape[1]
    start = 2 * block * lax.axis_index("c")
    for row, side in enumerate((start, 2 * block - start)):
        for q in range(2):
            sides[row * block : (row + 1) * block, q * block : (q + 1) * block] = band[
                q, pl.ds(side, block)
            ]
    middle = jnp.concatenate([band[q, block : 2 * block] for q in range(2)], axis=1)
    made[...] = jnp.dot(coeff[...], middle, preferred_element_type=jnp.float32)


def half_block(outer, partner, sides, made, half, copies, sems):
    nocc, block = outer.shape
    window = jnp.concatenate([outer[...], partner[...]], axis=1)
    whole = made[...] + jnp.dot(window, sides[...], preferred_element_type=jnp.float32)
    for q in range(2):
        half[q * nocc : (q + 1) * nocc] = whole[:, q * block : (q + 1) * block].astype(half.dtype)
    carried(*((half, copies.at[k], sems.at[k]) for k in range(4)))


def carried(*moves):
    copies = [pltpu.make_async_copy(*move) for move in moves]
    for copy in copies:
        copy.start()
    for copy in copies:
        copy.wait()


def tiles_of(columns, mine):
    block = mine.shape[2]
    made = lax.dot_general(
        jnp.concatenate([column[...] for column in columns], axis=1),
        jnp.concatenate([mine[k] for k in range(4)], axis=1),
        (((0,), (0,)), ((), ())),
        preferred_element_type=jnp.float32,
    )
    for k in range(4):
        yield (
            k,
            [
                made[j * block : (j + 1) * block, k * block : (k + 1) * block]
                for j in range(len(columns))
            ],
        )


def by_parity(store, tile):
    even = is_even()
    pl.when(even)(lambda: store(tile))
    pl.when(jnp.logical_not(even))(lambda: store(tile.T))


def first_tiles(own_other, near, mine, near_other, slices, patch, made, near_made, fetched, sems):
    cut = made.shape[4]
    core = lax.axis_index("c")
    own = mine.at[lax.axis_index("x")]
    fetch = pltpu.make_async_copy(near_other, fetched, sems.at[2])
    fetch.start()
    for k, tiles in tiles_of((own, own_other), mine):
        for side in range(2):
            for s in range(4):
                made[s, (core + side) % 2, 0, k] = tiles[side][s * cut : (s + 1) * cut]
    fetch.wait()
    for k, tiles in tiles_of((near, fetched), mine):
        for side in range(2):

            def put(tile, at=(core + side) % 2, k=k):
                for s in range(4):
                    made[s, at, 1, k] = tile[s * cut : (s + 1) * cut]
                    near_made[s, k, at] = tile[s * cut : (s + 1) * cut]

            by_parity(put, tiles[side])
    carried((made, slices, sems.at[0]), (near_made, patch.at[:, :, 0], sems.at[1]))


def far_tiles(far, far_other, mine, patch, whole, made, sems):
    cut = made.shape[3]
    core = lax.axis_index("c")
    for k, tiles in tiles_of((far, far_other), mine):
        for side in range(2):
            for s in range(4):
                made[s, k, (core + side) % 2] = tiles[side][s * cut : (s + 1) * cut]
    carried((made, whole.at[:, :, 1], sems.at[0]))


def near_summed(early, out):
    for c in range(2):
        for k in range(4):
            out[c, k] = early[0, c, 1, k] + early[1, c, 1, k] + early[2, c, 1, k] + early[3, c, 1, k]


def placed(early, mirrored, arrived, parts):
    zh = lax.axis_index("zh")
    toward = jnp.where(is_even(), 3, 1)
    homes = (lax.rem(zh + toward, 4), lax.rem(zh + 2, 4))
    for j in range(4):
        for c in range(2):
            parts[j, zh, c] = early[0, c, 0, j] + early[1, c, 0, j] + early[2, c, 0, j] + early[3, c, 0, j]
            parts[j, lax.rem(zh + 4 - toward, 4), c] = mirrored[c, j]
            for kind in range(2):
                parts[j, homes[kind], c] = (
                    arrived[0, j, kind, c]
                    + arrived[1, j, kind, c]
                    + arrived[2, j, kind, c]
                    + arrived[3, j, kind, c]
                )


def finished(pairs, total, out):
    block = out.shape[0]
    row = 8 * lax.axis_index("x") + 2 * lax.axis_index("zh") + lax.axis_index("c")
    first = 8 * lax.axis_index("zl") + 2 * lax.axis_index("y")
    straight = lax.rem(lax.axis_index("y") + 4 - lax.axis_index("zh"), 4) < 2
    kept = pairs[pl.ds(row, 1), :].astype(jnp.float32)
    places = lax.broadcasted_iota(jnp.int32, kept.shape, 1)
    for c in range(2):
        keep = jnp.sum(jnp.where(places == first + c, kept, 0.0), axis=1, keepdims=True)
        tile = total[0, :, c] + total[1, :, c] + total[2, :, c] + total[3, :, c]
        tile = tile.reshape(block, block) * keep

        @pl.when(straight)
        def _(tile=tile, c=c):
            out[:, c * block : (c + 1) * block] = tile

        @pl.when(jnp.logical_not(straight))
        def _(tile=tile, c=c):
            out[:, c * block : (c + 1) * block] = tile.T


def local(kernel, results, flops, *arrays, scratch=(), apart=False, filled=False):
    specs = [pl.BlockSpec(memory_space=pltpu.VMEM)] * len(arrays)
    if apart or filled:
        arrays = (*arrays[:-1], pltpu.with_memory_space_constraint(arrays[-1], pltpu.HBM))
        specs[-1] = pl.BlockSpec(memory_space=pltpu.HBM)
    shapes = [
        pltpu.HBM(shape, kind) if space == pltpu.HBM else jax.ShapeDtypeStruct(shape, kind)
        for shape, kind, space in results
    ]
    buffers = [pltpu.VMEM(shape, kind) for shape, kind in scratch]
    if any(space == pltpu.HBM for *_, space in results):
        buffers.append(pltpu.SemaphoreType.DMA((4,)))
    moved = sum(a.size * a.dtype.itemsize for a in arrays)
    moved += sum(math.prod(shape) * jnp.dtype(kind).itemsize for shape, kind, _ in results)
    return pl.pallas_call(
        kernel,
        out_shape=shapes,
        in_specs=specs,
        out_specs=[pl.BlockSpec(memory_space=space) for *_, space in results],
        scratch_shapes=buffers,
        input_output_aliases={len(arrays) - 1: 0} if filled else {},
        cost_estimate=pl.CostEstimate(flops=flops, bytes_accessed=moved, transcendentals=0),
        compiler_params=pltpu.CompilerParams(vmem_limit_bytes=2 * moved + (8 << 20)),
    )(*arrays)


def patch_sums(coeff, band, pairs):
    nocc, block = coeff.shape
    cut = block // 4

    count = lax.axis_size(ROW)
    partner = shifted(coeff, "c", 1)
    outward = [(r, r + 1) for r in range(1, count - 1, 2)]
    outer = lax.ppermute(coeff, ROW, outward + [(b, a) for a, b in outward])
    depth = band.shape[0] * nocc
    wide = band.shape[0] * block
    vmem, hbm = pltpu.VMEM, pltpu.HBM
    sides, made = local(
        own_part,
        [((2 * block, wide), jnp.bfloat16, vmem), ((nocc, wide), jnp.float32, vmem)],
        2 * nocc * block * wide,
        coeff,
        band,
    )
    half, copies = local(
        half_block,
        [((depth, block), jnp.bfloat16, vmem), ((4, depth, block), jnp.bfloat16, hbm)],
        4 * nocc * block * wide,
        outer,
        partner,
        sides,
        made,
    )

    near = lax.ppermute(half, ("zl", "zh"), ALONG_Z)
    mine = lax.all_to_all(copies, "x", split_axis=0, concat_axis=0, tiled=True)
    own_other = shifted(half, "c", 1)
    far = lax.ppermute(near, ("zl", "zh"), ALONG_Z)
    near_other = shifted(near, "c", 1)
    far_other = shifted(far, "c", 1)

    def summed(tiles, axes):
        return lax.all_to_all(tiles, axes, split_axis=0, concat_axis=0, tiled=True)

    work = 2 * depth * block * 8 * block
    patch_shape = (4, 4, 2, 2, cut, block)
    slices, patch = local(
        first_tiles,
        [((4, 2, 2, 4, cut, block), jnp.float32, hbm), (patch_shape, jnp.float32, hbm)],
        2 * work,
        own_other,
        near,
        mine,
        near_other,
        scratch=[
            ((4, 2, 2, 4, cut, block), jnp.float32),
            ((4, 4, 2, cut, block), jnp.float32),
            ((depth, block), jnp.bfloat16),
        ],
        apart=True,
    )
    early = summed(slices.reshape(8, 8 * cut, block), ("y", "c"))
    early = early.reshape(4, 2, 2, 4, cut, block)
    (mirrored,) = local(near_summed, [((2, 4, cut, block), jnp.float32, vmem)], 0, early)
    mirrored = lax.ppermute(mirrored, ("zl", "zh"), [(b, a) for a, b in ALONG_Z])
    (patch,) = local(
        far_tiles,
        [(patch_shape, jnp.float32, hbm)],
        work,
        far,
        far_other,
        mine,
        patch,
        scratch=[((4, 4, 2, cut, block), jnp.float32)],
        filled=True,
    )
    arrived = summed(patch.reshape(16, 4 * cut, block), ("y", "x"))
    arrived = arrived.reshape(4, 4, 2, 2, cut, block)
    (parts,) = local(
        placed, [((4, 4, 2, cut, block), jnp.float32, vmem)], 0, early, mirrored, arrived
    )
    total = lax.all_to_all(
        parts.reshape(16, 2 * cut, block), AUX, split_axis=0, concat_axis=0, tiled=True
    )
    total = total.reshape(4, 4, 2, cut, block)
    (out,) = local(
        finished, [((block, 2 * block), jnp.float32, vmem)], 0, pairs, total
    )
    return out


def solution(mesh):
    torus = Mesh(mesh.devices.reshape(4, 4, 4, 4, 2), ("zl", "y", "x", "zh", "c"))
    in_specs = (P(None, ROW), P(AUX, None, ROW), P())
    return jax.shard_map(
        patch_sums, mesh=torus, in_specs=in_specs, out_specs=P(ROW, AUX), check_vma=False
    )
```
